32 devices in a mesh: comp: 2 (over core), dom: 16 (over z, y, x).
Axes of the slice: x: 2, y: 2, z: 4, core: 2. Of those that a mesh axis runs over, the one named last changes fastest.
Arguments:
- surface_flux: float32 [6, 12, 131072], P(None, None, ('comp', 'dom')), may hold values from -8 to 8
- active_mask: int32 [131072], P(('comp', 'dom')), may hold values 0 or 1
- source_area: float32 [131072], P(('comp', 'dom')), may hold values from 0.5 to 30
- tile_targets: int32 [2048, 2], P(('comp', 'dom')), may hold values from 0 to 31, all different within a row
- remap_tiles: float32 [2048, 2, 64, 384], P(('comp', 'dom')), may hold values from -0.0625 to 0.0625
- ocean_flux: float32 [12, 12288], P(None, ('comp', 'dom')), may hold values from -6 to 6
- air_fraction: float32 [3, 12288], P(None, ('comp', 'dom')), may hold values from 0 to 1, as said below
- air_area: float32 [12288], P(('comp', 'dom')), may hold values from 0.5 to 30
Outputs:
- merged: float32 [12, 12288], P(None, ('comp', 'dom'))
- area_means: float32 [3, 12], replicated
The draws below stay inside these ranges and needn't reach their ends.
Inputs may be any that keep to these rules, and one draw needn't show every extreme that they name: `air_fraction`: the three fractions of a cell are positive and sum to one. `tile_targets`: the 2 targets of one source block differ.
All inputs are finite; a program needn't handle non-finite values. No bound on the sum of `active_mask` on one device may be relied on, other than what follows from the above.
Results may differ from the reference program's by a relative error of at most 0.000071.
Values sent between devices are 32-bit elements; how exact they have to be, the bound alone decides.
A program may use at most 64 MiB of HBM per device.

```python
import math
import jax
import jax.numpy as jnp
from jax import lax

FIELDS = 12
STEPS = 6
TOP = 2
BS = 64
SBLK = 64
ATM_DEV = 384
BLOCKS = 2048
SRC_CELLS = 131072
ATM_CELLS = 12288
N_COMP = 2
N_DOM = 16


def draw_surface_flux(key, part):
    subkeys = jax.random.split(key, 4)
    position = jnp.arange(SRC_CELLS, dtype=jnp.float32) / SRC_CELLS
    amplitude = jax.random.uniform(subkeys[0], (FIELDS, 1), jnp.float32, 0.5, 1.5)
    phase = jax.random.uniform(subkeys[1], (FIELDS, 1), jnp.float32, 0.0, 2.0 * math.pi)
    waves = 1.0 + (jnp.arange(FIELDS, dtype=jnp.int32) % 3).astype(jnp.float32)[:, None]
    offset = jax.random.uniform(subkeys[2], (FIELDS, 1), jnp.float32, -0.5, 0.5)
    trend = amplitude * jnp.cos(math.pi * waves * position[None, :] + phase) + offset
    noise = jax.random.normal(subkeys[3], (STEPS, FIELDS, SRC_CELLS), jnp.float32)
    return jnp.clip(trend[None, :, :] + noise, -8.0, 8.0)


def rising_area(key, total_cells):
    position = jnp.arange(total_cells, dtype=jnp.float32) / total_cells
    factor = jax.random.uniform(key, (total_cells,), jnp.float32, 0.5, 1.5)
    return (1.0 + 2.0 * position) * factor


def draw_source_area(key, part):
    return rising_area(jax.random.fold_in(key, 11), SRC_CELLS)


def draw_air_area(key, part):
    return rising_area(jax.random.fold_in(key, 23), ATM_CELLS)


def draw_air_fraction(key, part):
    shares = jax.random.uniform(key, (3, ATM_CELLS), jnp.float32, 0.1, 1.0)
    return shares / jnp.sum(shares, axis=0, keepdims=True)


def place_ends(result, key, smallest, largest):
    longest = result.shape.index(max(result.shape))
    spots = []
    for shift in (0, 1):
        where = [jax.random.randint(jax.random.fold_in(key, axis), (), 0, length) for axis, length in enumerate(result.shape)]
        where[longest] = (where[longest] + shift) % result.shape[longest]
        spots.append(tuple(where))
    return result.at[spots[0]].set(smallest).at[spots[1]].set(largest)


def shard_levels(own_key, shape, shards, smallest, largest):
    def one(axis_at, shards_of):
        heights = jax.random.uniform(jax.random.fold_in(jax.random.fold_in(own_key, 6), axis_at), (shards_of,), jnp.float32, smallest / len(shards), largest / len(shards))
        return jnp.repeat(jnp.exp(heights), shape[axis_at] // shards_of).reshape((-1,) + (1,) * (len(shape) - axis_at - 1))

    level = one(*shards[0])
    for cut in shards[1:]:
        level = level * one(*cut)
    return level


def different_ones(own_key, rows, number_of, top, lift):
    sequence = jax.random.permutation(jax.random.fold_in(own_key, 1), number_of)
    favour = sequence
    for power in range(3):
        favour = favour * favour // number_of
    favour = favour * lift // number_of
    lots = jax.random.randint(jax.random.fold_in(own_key, 2), (rows, number_of), 0, 4096) + favour
    holders = jax.random.permutation(jax.random.fold_in(own_key, 3), rows)[jnp.arange(number_of) % rows]
    lots = jnp.where(jnp.arange(rows)[:, None] == holders[None, :], 1 << 14, lots)
    priority = lots * number_of + jnp.arange(number_of)
    return lax.top_k(priority.astype(jnp.int32), top)[1].astype(jnp.int32)


def normal_values(rng, extent, spread, bound, cuts=(), kind=jnp.bfloat16):
    loudness = shard_levels(rng, extent, cuts, -0.22, 0.18) if cuts else 1.0
    result = jax.random.normal(rng, extent, jnp.float32) * spread * loudness
    return jnp.minimum(jnp.maximum(result, -bound), bound).astype(kind)


def setup_inputs(seed: int = 0) -> dict:
    streams_of = jax.random.split(jax.random.key(seed), 9)
    return {
        "surface_flux": draw_surface_flux(jax.random.fold_in(streams_of[8], 71), 0),
        "active_mask": place_ends((jax.random.randint(streams_of[1], (SRC_CELLS,), 0, 4) < 3).astype(jnp.int32), jax.random.fold_in(streams_of[1], 1), 0, 1),
        "source_area": draw_source_area(jax.random.fold_in(streams_of[8], 71), 0),
        "tile_targets": different_ones(streams_of[3], BLOCKS, N_COMP * N_DOM, TOP, 0),
        "remap_tiles": normal_values(streams_of[4], (BLOCKS, TOP, BS, ATM_DEV), (BS * SBLK * TOP) ** -0.5, 0.0625, ((0, 32),), jnp.float32),
        "ocean_flux": normal_values(streams_of[5], (FIELDS, ATM_CELLS), 1.0, 6.0, ((1, 32),), jnp.float32),
        "air_fraction": draw_air_fraction(jax.random.fold_in(streams_of[8], 71), 0),
        "air_area": draw_air_area(jax.random.fold_in(streams_of[8], 71), 0),
    }


def reference(surface_flux, active_mask, source_area, tile_targets, remap_tiles, ocean_flux, air_fraction, air_area):
    average = jnp.sum(surface_flux, axis=0) / STEPS
    weighted = average * (active_mask.astype(jnp.float32) * source_area)[None, :]
    blocks = weighted.reshape(FIELDS, BLOCKS, BS)
    contrib = jnp.einsum("fbs,btsa->btfa", blocks, remap_tiles, precision=lax.Precision.HIGHEST)
    contrib = contrib.reshape(BLOCKS * TOP, FIELDS, ATM_DEV)
    owner_total = N_COMP * N_DOM
    comp_of_block = (jnp.arange(BLOCKS, dtype=jnp.int32) // (SBLK * N_DOM)).astype(jnp.int32)
    segment = (comp_of_block[:, None] * owner_total + tile_targets).reshape(BLOCKS * TOP).astype(jnp.int32)
    summed = jax.ops.segment_sum(contrib, segment, num_segments=N_COMP * owner_total)
    summed = summed.reshape(N_COMP, owner_total, FIELDS, ATM_DEV).transpose(0, 2, 1, 3)
    remapped = summed.reshape(N_COMP, FIELDS, ATM_CELLS) / air_area[None, None, :]
    merged = air_fraction[0][None, :] * remapped[0] + air_fraction[1][None, :] * remapped[1] + air_fraction[2][None, :] * ocean_flux
    surface_num = jnp.sum(weighted.reshape(FIELDS, N_COMP, SRC_CELLS // N_COMP), axis=2).T
    surface_den = jnp.sum(source_area.reshape(N_COMP, SRC_CELLS // N_COMP), axis=1)
    air_num = jnp.sum(merged * air_area[None, :], axis=1)
    air_den = jnp.sum(air_area)
    area_means = jnp.concatenate([surface_num / surface_den[:, None], (air_num / air_den)[None, :]], axis=0)
    return merged, area_means
```

```python
import functools

import jax
import jax.numpy as jnp
from jax import lax
from jax.experimental import pallas as pl
from jax.experimental.pallas import tpu as pltpu
from jax.sharding import PartitionSpec as P

MESH = pl.DeviceIdType.MESH
F32 = jnp.float32
BF16 = jnp.bfloat16
CHUNKS = 8


def split(x):
    hi = x.astype(BF16)
    lo = (x - hi.astype(F32)).astype(BF16)
    return hi, lo


def kernel(
    groups,
    domains,
    flux_hbm,
    mask_ref,
    area_ref,
    targets_ref,
    tiles_hbm,
    ocean_ref,
    fraction_ref,
    air_ref,
    merged_ref,
    means_ref,
    flux,
    tiles,
    weighted,
    contrib,
    picks,
    rows_out,
    rows_in,
    summed,
    partner_in,
    outgoing,
    incoming,
    air_rows,
    stat_out,
    stat_in,
    flux_sem,
    tile_sem,
    row_send,
    row_recv,
    stat_send,
    stat_recv,
    pair_send,
    pair_recv,
    main_send,
    main_recv,
):
    steps, fields, cells = flux.shape
    blocks, slots, block_cells, air_cells = tiles.shape
    owners = groups * domains
    per_chunk = blocks // CHUNKS
    lane_tiles = air_cells // 128
    tile_count = blocks * slots
    comp = lax.axis_index("comp")
    dom = lax.axis_index("dom")
    me = comp * domains + dom
    other = 1 - comp

    flux_copy = pltpu.make_async_copy(flux_hbm, flux, flux_sem)
    flux_copy.start()
    tile_copies = []
    for i in range(CHUNKS):
        part = pl.ds(i * per_chunk, per_chunk)
        copy = pltpu.make_async_copy(tiles_hbm.at[part], tiles.at[part], tile_sem.at[i])
        copy.start()
        tile_copies.append(copy)

    barrier = pltpu.get_barrier_semaphore()

    def device(p):
        return (p // domains, p % domains)

    @pl.loop(1, owners)
    def _(k):
        pl.semaphore_signal(
            barrier, inc=1, device_id=device((me + k) % owners), device_id_type=MESH
        )

    for c in range(groups):
        rows_out[c, :, pl.ds(0, air_cells)] = fraction_ref[pl.ds(c, 1), :]
        rows_out[c, :, pl.ds(air_cells, air_cells)] = air_ref[...]
    rows_in[me] = rows_out[comp]
    pl.semaphore_wait(barrier, owners - 1)

    def row_copy(k):
        p = (me + k) % owners
        return pltpu.make_async_remote_copy(
            src_ref=rows_out.at[p // domains],
            dst_ref=rows_in.at[me],
            send_sem=row_send.at[k],
            recv_sem=row_recv.at[me],
            device_id=device(p),
            device_id_type=MESH,
        )

    @pl.loop(1, owners)
    def _(k):
        row_copy(k).start()

    flux_copy.wait()
    weighted[pl.ds(8, 8), :] = jnp.zeros((8, cells), F32)
    width = 512

    def weigh(i, carry):
        total, area_total = carry
        part = pl.ds(pl.multiple_of(i * width, width), width)
        value = flux[0, :, part]
        for s in range(1, steps):
            value = value + flux[s, :, part]
        area = area_ref[:, part]
        value = (value / steps) * (mask_ref[:, part].astype(F32) * area)
        weighted[pl.ds(0, fields), part] = value
        return total + value, area_total + area

    total, area_total = lax.fori_loop(
        0,
        cells // width,
        weigh,
        (jnp.zeros((fields, width), F32), jnp.zeros((1, width), F32)),
    )
    surface_num = jnp.sum(total, axis=1, keepdims=True)
    surface_den = jnp.sum(area_total)

    lane = lax.broadcasted_iota(jnp.int32, (16, 128), 1)
    first = lane < block_cells
    blank = jnp.zeros((16, 128), BF16)

    def pair(j, carry):
        cell = pl.ds(pl.multiple_of(j * 128, 128), 128)
        w = weighted[:, cell]
        lhs = []
        for keep in (first, ~first):
            hi, lo = split(jnp.where(keep, w, 0.0))
            lhs.append(jnp.concatenate([hi, hi], axis=1))
            lhs.append(jnp.concatenate([lo, blank], axis=1))
        left = jnp.concatenate(lhs, axis=0)
        for t in range(slots):
            weights = tiles[pl.ds(2 * j, 2), t].reshape(2 * block_cells, air_cells)
            hi, lo = split(weights)
            right = jnp.concatenate([hi, lo], axis=0)
            r = jnp.dot(left, right, preferred_element_type=F32)
            even = r[0:16] + r[16:32]
            odd = r[32:48] + r[48:64]
            base = pl.multiple_of((t * blocks + 2 * j) * 16, 32)
            for q in range(lane_tiles):
                cut = slice(q * 128, (q + 1) * 128)
                contrib[q, pl.ds(base, 16), :] = even[:, cut]
                contrib[q, pl.ds(base + 16, 16), :] = odd[:, cut]
        return carry

    pairs = per_chunk // 2
    for i in range(CHUNKS):
        tile_copies[i].wait()
        lax.fori_loop(i * pairs, (i + 1) * pairs, pair, 0)

    picks[:, pl.ds(0, blocks)] = targets_ref[...]
    picks[:, pl.ds(blocks, blocks)] = targets_ref[...]
    picked = jnp.where(
        lax.broadcasted_iota(jnp.int32, (1, tile_count), 1) < blocks,
        picks[pl.ds(0, 1), :],
        picks[pl.ds(1, 1), :],
    )
    owner_ids = lax.broadcasted_iota(jnp.int32, (owners, tile_count), 0)
    selector = jnp.where(owner_ids == picked, 1.0, 0.0).astype(BF16)
    selector = jnp.concatenate([selector, selector], axis=1)

    @pl.loop(1, owners)
    def _(k):
        p = (me + k) % owners
        pltpu.make_async_remote_copy(
            src_ref=rows_out.at[0],
            dst_ref=rows_in.at[p],
            send_sem=row_send.at[k],
            recv_sem=row_recv.at[p],
            device_id=device(p),
            device_id_type=MESH,
        ).wait_recv()

    rows = rows_in[:, 0, :]
    fraction = rows[:, :air_cells]
    scale = fraction / rows[:, air_cells:]

    air_rows[...] = jnp.zeros(air_rows.shape, F32)

    def gather(f, carry):
        right = []
        for q in range(lane_tiles):
            hi, lo = split(contrib[q, pl.ds(f, tile_count, stride=16), :])
            right.append(jnp.concatenate([hi, lo], axis=0))
        s = jnp.dot(selector, jnp.concatenate(right, axis=1), preferred_element_type=F32)
        summed[f] = s * scale
        air_rows[pl.ds(f, 1), :] = jnp.sum(s * fraction, axis=0, keepdims=True)
        return carry

    lax.fori_loop(0, fields, gather, 0)

    pair_copy = pltpu.make_async_remote_copy(
        src_ref=summed.at[:, pl.ds(pl.multiple_of(other * domains, 8), domains), :],
        dst_ref=partner_in,
        send_sem=pair_send,
        recv_sem=pair_recv,
        device_id=(other, dom),
        device_id_type=MESH,
    )
    pair_copy.start()

    ocean = fraction_ref[pl.ds(2, 1), :] * ocean_ref[...]
    air_num = jnp.sum(air_rows[pl.ds(0, fields), :] + air_ref[...] * ocean, axis=1, keepdims=True)
    air_den = jnp.sum(air_ref[...])
    spot = lax.broadcasted_iota(jnp.int32, (fields, 128), 1)
    line = lax.broadcasted_iota(jnp.int32, (fields, 128), 0)
    stat = jnp.where(spot == line + 16 * comp, surface_num, 0.0)
    stat = stat + jnp.where(spot == line + 16 * groups, air_num, 0.0)
    stat = jnp.sum(stat, axis=0, keepdims=True)
    spot = lax.broadcasted_iota(jnp.int32, (1, 128), 1)
    dens = 16 * (groups + 1)
    stat = stat + jnp.where(spot == dens + comp, surface_den, 0.0)
    stat = stat + jnp.where(spot == dens + groups, air_den, 0.0)
    stat_out[...] = stat
    stat_in[me] = stat

    def stat_copy(k, slot):
        return pltpu.make_async_remote_copy(
            src_ref=stat_out,
            dst_ref=stat_in.at[slot],
            send_sem=stat_send.at[k],
            recv_sem=stat_recv.at[slot],
            device_id=device((me + k) % owners),
            device_id_type=MESH,
        )

    @pl.loop(1, owners)
    def _(k):
        stat_copy(k, me).start()

    pair_copy.wait()
    own = pl.ds(pl.multiple_of(comp * domains, 8), domains)
    for f in range(fields):
        outgoing[:, f, :] = summed[f, own, :] + partner_in[f]

    def main_copy(k, slot):
        p = (dom + k) % domains
        return pltpu.make_async_remote_copy(
            src_ref=outgoing.at[p],
            dst_ref=incoming.at[slot],
            send_sem=main_send.at[k],
            recv_sem=main_recv.at[slot],
            device_id=(comp, p),
            device_id_type=MESH,
        )

    @pl.loop(1, domains)
    def _(k):
        main_copy(k, dom).start()

    merged_ref[...] = ocean + outgoing[dom]

    @pl.loop(1, owners)
    def _(k):
        stat_copy(k, (me + k) % owners).wait_recv()

    stat = jnp.sum(stat_in[...], axis=0)
    for c in range(groups + 1):
        den = jnp.sum(jnp.where(spot == dens + c, stat, 0.0))
        moved = stat if c == 0 else pltpu.roll(stat, 128 - 16 * c, 1)
        means_ref[pl.ds(c, 1), :] = moved[:, :fields] / den

    @pl.loop(1, domains)
    def _(k):
        slot = (dom + k) % domains
        main_copy(k, slot).wait_recv()
        merged_ref[...] += incoming[slot]

    @pl.loop(1, owners)
    def _(k):
        row_copy(k).wait_send()
        stat_copy(k, me).wait_send()

    @pl.loop(1, domains)
    def _(k):
        main_copy(k, dom).wait_send()


def on_device(
    surface_flux,
    active_mask,
    source_area,
    tile_targets,
    remap_tiles,
    ocean_flux,
    air_fraction,
    air_area,
):
    groups = lax.axis_size("comp")
    domains = lax.axis_size("dom")
    owners = groups * domains
    fields = surface_flux.shape[1]
    cells = surface_flux.shape[2]
    blocks, slots, block_cells, air_cells = remap_tiles.shape
    vmem = pl.BlockSpec(memory_space=pltpu.VMEM)
    hbm = pl.BlockSpec(memory_space=pl.ANY)
    dma = pltpu.SemaphoreType.DMA
    return pl.pallas_call(
        functools.partial(kernel, groups, domains),
        out_shape=(
            jax.ShapeDtypeStruct((fields, air_cells), F32),
            jax.ShapeDtypeStruct((groups + 1, fields), F32),
        ),
        in_specs=[hbm, vmem, vmem, vmem, hbm, vmem, vmem, vmem],
        out_specs=(vmem, vmem),
        scratch_shapes=[
            pltpu.VMEM(surface_flux.shape, F32),
            pltpu.VMEM(remap_tiles.shape, F32),
            pltpu.VMEM((16, cells), F32),
            pltpu.VMEM((air_cells // 128, blocks * slots * 16, 128), F32),
            pltpu.VMEM((slots, blocks * slots), jnp.int32),
            pltpu.VMEM((groups, 1, 2 * air_cells), F32),
            pltpu.VMEM((owners, 1, 2 * air_cells), F32),
            pltpu.VMEM((fields, owners, air_cells), F32),
            pltpu.VMEM((fields, domains, air_cells), F32),
            pltpu.VMEM((domains, fields, air_cells), F32),
            pltpu.VMEM((domains, fields, air_cells), F32),
            pltpu.VMEM((16, air_cells), F32),
            pltpu.VMEM((1, 128), F32),
            pltpu.VMEM((owners, 1, 128), F32),
            dma,
            dma((CHUNKS,)),
            dma((owners,)),
            dma((owners,)),
            dma((owners,)),
            dma((owners,)),
            dma,
            dma,
            dma((domains,)),
            dma((domains,)),
        ],
        compiler_params=pltpu.CompilerParams(
            collective_id=0, has_side_effects=True, vmem_limit_bytes=60 * 1024 * 1024
        ),
    )(
        surface_flux,
        active_mask.reshape(1, cells),
        source_area.reshape(1, cells),
        tile_targets.T,
        remap_tiles,
        ocean_flux,
        air_fraction,
        air_area.reshape(1, air_cells),
    )


def solution(mesh):
    in_specs = (
        P(None, None, ("comp", "dom")),
        P(("comp", "dom")),
        P(("comp", "dom")),
        P(("comp", "dom"), None),
        P(("comp", "dom"), None, None, None),
        P(None, ("comp", "dom")),
        P(None, ("comp", "dom")),
        P(("comp", "dom")),
    )
    out_specs = (P(None, ("comp", "dom")), P())
    return jax.shard_map(
        on_device, mesh=mesh, in_specs=in_specs, out_specs=out_specs, check_vma=False
    )
```

```python
import functools

import jax
import jax.numpy as jnp
from jax import lax
from jax.experimental import pallas as pl
from jax.experimental.pallas import tpu as pltpu
from jax.sharding import PartitionSpec as P

MESH = pl.DeviceIdType.MESH
F32 = jnp.float32
BF16 = jnp.bfloat16
CHUNKS = 8
DEPTH = 4
UNROLL = 4


def split(x):
    hi = x.astype(BF16)
    lo = (x - hi.astype(F32)).astype(BF16)
    return hi, lo


def kernel(
    groups,
    domains,
    flux_hbm,
    mask_ref,
    area_ref,
    targets_ref,
    tiles_hbm,
    ocean_ref,
    fraction_ref,
    air_ref,
    merged_ref,
    means_ref,
    flux,
    tiles,
    weighted,
    contrib,
    picks,
    rows_out,
    rows_own,
    rows_in,
    summed,
    partner_in,
    outgoing_a,
    outgoing_b,
    incoming_a,
    incoming_b,
    air_rows,
    stat_out,
    stat_other,
    stat_sum,
    stat_in,
    flux_sem,
    tile_sem,
    row_pair_send,
    row_pair_recv,
    row_send,
    row_recv,
    stat_pair_send,
    stat_pair_recv,
    stat_send,
    stat_recv,
    pair_send,
    pair_recv,
    main_send,
    main_recv,
):
    steps, fields, cells = flux.shape
    blocks, slots, block_cells, air_cells = tiles.shape
    owners = groups * domains
    per_chunk = blocks // CHUNKS
    lane_tiles = air_cells // 128
    tile_count = blocks * slots
    comp = lax.axis_index("comp")
    dom = lax.axis_index("dom")
    other = 1 - comp
    outgoing = (outgoing_a, outgoing_b)
    incoming = (incoming_a, incoming_b)

    flux_copy = pltpu.make_async_copy(flux_hbm, flux, flux_sem)
    flux_copy.start()
    tile_copies = []
    for i in range(CHUNKS):
        part = pl.ds(i * per_chunk, per_chunk)
        copy = pltpu.make_async_copy(tiles_hbm.at[part], tiles.at[part], tile_sem.at[i])
        if i < DEPTH:
            copy.start()
        tile_copies.append(copy)

    barrier = pltpu.get_barrier_semaphore()

    def peer(k):
        p = dom + k
        return jnp.where(p >= domains, p - domains, p)

    peers = list(range(1, domains))
    pl.semaphore_signal(barrier, inc=1, device_id=(other, dom), device_id_type=MESH)
    for k in peers:
        pl.semaphore_signal(barrier, inc=1, device_id=(comp, peer(k)), device_id_type=MESH)

    air = air_ref[...].reshape(1, air_cells)
    for c in range(groups):
        rows_out[c, :, pl.ds(0, air_cells)] = fraction_ref[pl.ds(c, 1), :]
        rows_out[c, :, pl.ds(air_cells, air_cells)] = air
    rows_own[comp] = rows_out[comp]

    row_pair = pltpu.make_async_remote_copy(
        src_ref=rows_out.at[other],
        dst_ref=rows_own.at[comp],
        send_sem=row_pair_send,
        recv_sem=row_pair_recv,
        device_id=(other, dom),
        device_id_type=MESH,
    )

    def row_copy(k, slot):
        return pltpu.make_async_remote_copy(
            src_ref=rows_own,
            dst_ref=rows_in.at[:, slot],
            send_sem=row_send.at[k],
            recv_sem=row_recv.at[slot],
            device_id=(comp, peer(k)),
            device_id_type=MESH,
        )

    pl.semaphore_wait(barrier, domains)
    row_pair.start()
    row_pair.wait()
    for k in peers:
        row_copy(k, dom).start()
    flux_copy.wait()
    weighted[pl.ds(8, 8), :] = jnp.zeros((8, cells), F32)
    width = 512

    def weigh(i, carry):
        total, area_total = carry
        part = pl.ds(pl.multiple_of(i * width, width), width)
        value = flux[0, :, part]
        for s in range(1, steps):
            value = value + flux[s, :, part]
        area = area_ref[:, part]
        value = (value / steps) * (mask_ref[:, part].astype(F32) * area)
        weighted[pl.ds(0, fields), part] = value
        return total + value, area_total + area

    total, area_total = lax.fori_loop(
        0,
        cells // width,
        weigh,
        (jnp.zeros((fields, width), F32), jnp.zeros((1, width), F32)),
        unroll=2,
    )
    surface_num = jnp.sum(total, axis=1, keepdims=True)
    surface_den = jnp.sum(area_total)

    lane = lax.broadcasted_iota(jnp.int32, (16, 128), 1)
    first = lane < block_cells
    blank = jnp.zeros((16, 128), BF16)

    def pair(j, carry):
        cell = pl.ds(pl.multiple_of(j * 128, 128), 128)
        w = weighted[:, cell]
        lhs = []
        for keep in (first, ~first):
            hi, lo = split(jnp.where(keep, w, 0.0))
            lhs.append(jnp.concatenate([hi, hi], axis=1))
            lhs.append(jnp.concatenate([lo, blank], axis=1))
        left = jnp.concatenate(lhs, axis=0)
        for t in range(slots):
            weights = tiles[pl.ds(2 * j, 2), t].reshape(2 * block_cells, air_cells)
            hi, lo = split(weights)
            right = jnp.concatenate([hi, lo], axis=0)
            r = jnp.dot(left, right, preferred_element_type=F32)
            even = r[0:16] + r[16:32]
            odd = r[32:48] + r[48:64]
            base = pl.multiple_of((t * blocks + 2 * j) * 16, 32)
            for q in range(lane_tiles):
                cut = slice(q * 128, (q + 1) * 128)
                contrib[q, pl.ds(base, 16), :] = even[:, cut]
                contrib[q, pl.ds(base + 16, 16), :] = odd[:, cut]
        return carry

    pairs = per_chunk // 2
    for i in range(CHUNKS):
        tile_copies[i].wait()
        if i + DEPTH < CHUNKS:
            tile_copies[i + DEPTH].start()
        lax.fori_loop(i * pairs, (i + 1) * pairs, pair, 0, unroll=UNROLL)

    picks[:, pl.ds(0, blocks)] = targets_ref[...]
    picks[:, pl.ds(blocks, blocks)] = targets_ref[...]
    picked = jnp.where(
        lax.broadcasted_iota(jnp.int32, (1, tile_count), 1) < blocks,
        picks[pl.ds(0, 1), :],
        picks[pl.ds(1, 1), :],
    )
    owner_ids = lax.broadcasted_iota(jnp.int32, (owners, tile_count), 0)
    selector = jnp.where(owner_ids == picked, 1.0, 0.0).astype(BF16)
    selector = jnp.concatenate([selector, selector], axis=1)

    air_rows[...] = jnp.zeros(air_rows.shape, F32)

    rows_in[:, pl.ds(dom, 1)] = rows_own[...].reshape(groups, 1, 1, 2 * air_cells)
    for k in peers:
        row_copy(k, peer(k)).wait_recv()

    rows = rows_in[...].reshape(owners, 2 * air_cells)
    fraction = rows[:, :air_cells]
    scale = fraction / rows[:, air_cells:]

    def gather(f, carry):
        right = []
        for q in range(lane_tiles):
            hi, lo = split(contrib[q, pl.ds(f, tile_count, stride=16), :])
            right.append(jnp.concatenate([hi, lo], axis=0))
        s = jnp.dot(selector, jnp.concatenate(right, axis=1), preferred_element_type=F32)
        summed[f] = s * scale
        air_rows[pl.ds(f, 1), :] = jnp.sum(s * fraction, axis=0, keepdims=True)
        return carry

    far = pl.ds(pl.multiple_of(other * domains, 8), domains)
    cuts = [(0, 8), (8, fields - 8)]
    pair_copies = []
    for n, (low, count) in enumerate(cuts):
        lax.fori_loop(low, low + count, gather, 0, unroll=4)
        part = pl.ds(low, count)
        copy = pltpu.make_async_remote_copy(
            src_ref=summed.at[part, far],
            dst_ref=partner_in.at[part],
            send_sem=pair_send.at[n],
            recv_sem=pair_recv.at[n],
            device_id=(other, dom),
            device_id_type=MESH,
        )
        copy.start()
        pair_copies.append(copy)
    ocean = fraction_ref[pl.ds(2, 1), :] * ocean_ref[...]
    air_num = jnp.sum(air_rows[pl.ds(0, fields), :] + air * ocean, axis=1, keepdims=True)
    air_den = jnp.sum(air)
    spot = lax.broadcasted_iota(jnp.int32, (fields, 128), 1)
    line = lax.broadcasted_iota(jnp.int32, (fields, 128), 0)
    stat = jnp.where(spot == line + 16 * comp, surface_num, 0.0)
    stat = stat + jnp.where(spot == line + 16 * groups, air_num, 0.0)
    stat = jnp.sum(stat, axis=0, keepdims=True)
    spot = lax.broadcasted_iota(jnp.int32, (1, 128), 1)
    dens = 16 * (groups + 1)
    stat = stat + jnp.where(spot == dens + comp, surface_den, 0.0)
    stat = stat + jnp.where(spot == dens + groups, air_den, 0.0)
    stat_out[...] = stat
    stat_pair = pltpu.make_async_remote_copy(
        src_ref=stat_out,
        dst_ref=stat_other,
        send_sem=stat_pair_send,
        recv_sem=stat_pair_recv,
        device_id=(other, dom),
        device_id_type=MESH,
    )
    stat_pair.start()

    def stat_copy(k, slot):
        return pltpu.make_async_remote_copy(
            src_ref=stat_sum,
            dst_ref=stat_in.at[slot],
            send_sem=stat_send.at[k],
            recv_sem=stat_recv.at[slot],
            device_id=(comp, peer(k)),
            device_id_type=MESH,
        )

    own = pl.ds(pl.multiple_of(comp * domains, 8), domains)

    def main_copy(n, k, slot):
        p = peer(k)
        return pltpu.make_async_remote_copy(
            src_ref=outgoing[n].at[p],
            dst_ref=incoming[n].at[slot],
            send_sem=main_send.at[n, k],
            recv_sem=main_recv.at[n, slot],
            device_id=(comp, p),
            device_id_type=MESH,
        )

    def send_group(n):
        low, count = cuts[n]
        pair_copies[n].wait()
        for f in range(low, low + count):
            outgoing[n][:, f - low, :] = summed[f, own, :] + partner_in[f]
        for k in peers:
            main_copy(n, k, dom).start()

    send_group(0)
    stat_pair.wait()
    stat = stat_out[...] + stat_other[...]
    stat_sum[...] = stat
    stat_in[dom] = stat
    for k in peers:
        stat_copy(k, dom).start()
    send_group(1)

    for n, (low, count) in enumerate(cuts):
        merged_ref[pl.ds(low, count), :] = ocean[low : low + count] + outgoing[n][dom]

    for n, (low, count) in enumerate(cuts):
        part = pl.ds(low, count)
        total = merged_ref[part, :]
        for k in peers:
            slot = peer(k)
            main_copy(n, k, slot).wait_recv()
            total = total + incoming[n][slot]
        merged_ref[part, :] = total
    for k in peers:
        stat_copy(k, peer(k)).wait_recv()

    stat = jnp.sum(stat_in[...], axis=0)
    for c in range(groups + 1):
        den = jnp.sum(jnp.where(spot == dens + c, stat, 0.0))
        moved = stat if c == 0 else pltpu.roll(stat, 128 - 16 * c, 1)
        means_ref[pl.ds(c, 1), :] = moved[:, :fields] / den

    for k in peers:
        row_copy(k, dom).wait_send()
        main_copy(0, k, dom).wait_send()
        main_copy(1, k, dom).wait_send()
        stat_copy(k, dom).wait_send()


def finish(merged_in, means_in, merged_ref, means_ref):
    merged_ref[...] = merged_in[...]
    means_ref[...] = means_in[...]


def on_device(
    surface_flux,
    active_mask,
    source_area,
    tile_targets,
    remap_tiles,
    ocean_flux,
    air_fraction,
    air_area,
):
    groups = lax.axis_size("comp")
    domains = lax.axis_size("dom")
    owners = groups * domains
    fields = surface_flux.shape[1]
    cells = surface_flux.shape[2]
    blocks, slots, block_cells, air_cells = remap_tiles.shape
    vmem = pl.BlockSpec(memory_space=pltpu.VMEM)
    hbm = pl.BlockSpec(memory_space=pl.ANY)
    dma = pltpu.SemaphoreType.DMA
    shapes = (
        jax.ShapeDtypeStruct((fields, air_cells), F32),
        jax.ShapeDtypeStruct((groups + 1, fields), F32),
    )
    parts = pl.pallas_call(
        functools.partial(kernel, groups, domains),
        out_shape=shapes,
        in_specs=[hbm, vmem, vmem, vmem, hbm, vmem, vmem, vmem],
        out_specs=(vmem, vmem),
        scratch_shapes=[
            pltpu.VMEM(surface_flux.shape, F32),
            pltpu.VMEM(remap_tiles.shape, F32),
            pltpu.VMEM((16, cells), F32),
            pltpu.VMEM((air_cells // 128, blocks * slots * 16, 128), F32),
            pltpu.VMEM((slots, blocks * slots), jnp.int32),
            pltpu.VMEM((groups, 1, 2 * air_cells), F32),
            pltpu.VMEM((groups, 1, 2 * air_cells), F32),
            pltpu.VMEM((groups, domains, 1, 2 * air_cells), F32),
            pltpu.VMEM((fields, owners, air_cells), F32),
            pltpu.VMEM((fields, domains, air_cells), F32),
            pltpu.VMEM((domains, 8, air_cells), F32),
            pltpu.VMEM((domains, fields - 8, air_cells), F32),
            pltpu.VMEM((domains, 8, air_cells), F32),
            pltpu.VMEM((domains, fields - 8, air_cells), F32),
            pltpu.VMEM((16, air_cells), F32),
            pltpu.VMEM((1, 128), F32),
            pltpu.VMEM((1, 128), F32),
            pltpu.VMEM((1, 128), F32),
            pltpu.VMEM((domains, 1, 128), F32),
            dma,
            dma((CHUNKS,)),
            dma,
            dma,
            dma((domains,)),
            dma((domains,)),
            dma,
            dma,
            dma((domains,)),
            dma((domains,)),
            dma((2,)),
            dma((2,)),
            dma((2, domains)),
            dma((2, domains)),
        ],
        compiler_params=pltpu.CompilerParams(
            collective_id=0, has_side_effects=True, vmem_limit_bytes=60 * 1024 * 1024
        ),
    )(
        surface_flux,
        active_mask.reshape(1, cells),
        source_area.reshape(1, cells),
        tile_targets.T,
        remap_tiles,
        ocean_flux,
        air_fraction,
        air_area,
    )
    return pl.pallas_call(
        finish, out_shape=shapes, in_specs=[vmem, vmem], out_specs=(vmem, vmem)
    )(*parts)


def solution(mesh):
    in_specs = (
        P(None, None, ("comp", "dom")),
        P(("comp", "dom")),
        P(("comp", "dom")),
        P(("comp", "dom"), None),
        P(("comp", "dom"), None, None, None),
        P(None, ("comp", "dom")),
        P(None, ("comp", "dom")),
        P(("comp", "dom")),
    )
    out_specs = (P(None, ("comp", "dom")), P())
    return jax.shard_map(
        on_device, mesh=mesh, in_specs=in_specs, out_specs=out_specs, check_vma=False
    )
```

```python
import functools

import jax
import jax.numpy as jnp
from jax import lax
from jax.experimental import pallas as pl
from jax.experimental.pallas import tpu as pltpu
from jax.sharding import PartitionSpec as P

MESH = pl.DeviceIdType.MESH
F32 = jnp.float32
BF16 = jnp.bfloat16
CHUNKS = 8
DEPTH = 4
UNROLL = 4


def split(x):
    hi = x.astype(BF16)
    lo = (x - hi.astype(F32)).astype(BF16)
    return hi, lo


def kernel(
    groups,
    domains,
    flux_hbm,
    mask_ref,
    area_ref,
    targets_ref,
    tiles_hbm,
    ocean_ref,
    fraction_ref,
    air_ref,
    merged_ref,
    means_ref,
    flux,
    tiles,
    weighted,
    contrib,
    picks,
    rows_out,
    rows_own,
    rows_in,
    summed,
    partner_in,
    outgoing_a,
    outgoing_b,
    incoming_a,
    incoming_b,
    air_rows,
    stat_out,
    stat_other,
    stat_sum,
    stat_in,
    flux_sem,
    tile_sem,
    row_pair_send,
    row_pair_recv,
    row_send,
    row_recv,
    stat_pair_send,
    stat_pair_recv,
    stat_send,
    stat_recv,
    pair_send,
    pair_recv,
    main_send,
    main_recv,
):
    steps, fields, cells = flux.shape
    blocks, slots, block_cells, air_cells = tiles.shape
    owners = groups * domains
    per_chunk = blocks // CHUNKS
    lane_tiles = air_cells // 128
    tile_count = blocks * slots
    comp = lax.axis_index("comp")
    dom = lax.axis_index("dom")
    other = 1 - comp
    outgoing = (outgoing_a, outgoing_b)
    incoming = (incoming_a, incoming_b)

    flux_copy = pltpu.make_async_copy(flux_hbm, flux, flux_sem)
    flux_copy.start()
    tile_copies = []
    for i in range(CHUNKS):
        part = pl.ds(i * per_chunk, per_chunk)
        copy = pltpu.make_async_copy(tiles_hbm.at[part], tiles.at[part], tile_sem.at[i])
        if i < DEPTH:
            copy.start()
        tile_copies.append(copy)

    barrier = pltpu.get_barrier_semaphore()

    def peer(k):
        p = dom + jnp.where(comp == 0, k, domains - k)
        return jnp.where(p >= domains, p - domains, p)

    peers = list(range(1, domains))
    pl.semaphore_signal(barrier, inc=1, device_id=(other, dom), device_id_type=MESH)
    for k in peers:
        pl.semaphore_signal(barrier, inc=1, device_id=(comp, peer(k)), device_id_type=MESH)

    air = air_ref[...].reshape(1, air_cells)
    for c in range(groups):
        rows_out[c, :, pl.ds(0, air_cells)] = fraction_ref[pl.ds(c, 1), :]
        rows_out[c, :, pl.ds(air_cells, air_cells)] = air
    rows_own[comp] = rows_out[comp]

    row_pair = pltpu.make_async_remote_copy(
        src_ref=rows_out.at[other],
        dst_ref=rows_own.at[comp],
        send_sem=row_pair_send,
        recv_sem=row_pair_recv,
        device_id=(other, dom),
        device_id_type=MESH,
    )

    def row_copy(k, slot):
        return pltpu.make_async_remote_copy(
            src_ref=rows_own,
            dst_ref=rows_in.at[:, slot],
            send_sem=row_send.at[k],
            recv_sem=row_recv.at[slot],
            device_id=(comp, peer(k)),
            device_id_type=MESH,
        )

    pl.semaphore_wait(barrier, domains)
    row_pair.start()
    row_pair.wait()
    for k in peers:
        row_copy(k, dom).start()
    flux_copy.wait()
    weighted[pl.ds(8, 8), :] = jnp.zeros((8, cells), F32)
    width = 512

    def weigh(i, carry):
        total, area_total = carry
        part = pl.ds(pl.multiple_of(i * width, width), width)
        value = flux[0, :, part]
        for s in range(1, steps):
            value = value + flux[s, :, part]
        area = area_ref[:, part]
        value = (value / steps) * (mask_ref[:, part].astype(F32) * area)
        weighted[pl.ds(0, fields), part] = value
        return total + value, area_total + area

    total, area_total = lax.fori_loop(
        0,
        cells // width,
        weigh,
        (jnp.zeros((fields, width), F32), jnp.zeros((1, width), F32)),
        unroll=2,
    )
    surface_num = jnp.sum(total, axis=1, keepdims=True)
    surface_den = jnp.sum(area_total)

    lane = lax.broadcasted_iota(jnp.int32, (16, 128), 1)
    first = lane < block_cells
    blank = jnp.zeros((16, 128), BF16)

    def pair(j, carry):
        cell = pl.ds(pl.multiple_of(j * 128, 128), 128)
        w = weighted[:, cell]
        lhs = []
        for keep in (first, ~first):
            hi, lo = split(jnp.where(keep, w, 0.0))
            lhs.append(jnp.concatenate([hi, hi], axis=1))
            lhs.append(jnp.concatenate([lo, blank], axis=1))
        left = jnp.concatenate(lhs, axis=0)
        for t in range(slots):
            weights = tiles[pl.ds(2 * j, 2), t].reshape(2 * block_cells, air_cells)
            hi, lo = split(weights)
            right = jnp.concatenate([hi, lo], axis=0)
            r = jnp.dot(left, right, preferred_element_type=F32)
            even = r[0:16] + r[16:32]
            odd = r[32:48] + r[48:64]
            base = pl.multiple_of((t * blocks + 2 * j) * 16, 32)
            for q in range(lane_tiles):
                cut = slice(q * 128, (q + 1) * 128)
                contrib[q, pl.ds(base, 16), :] = even[:, cut]
                contrib[q, pl.ds(base + 16, 16), :] = odd[:, cut]
        return carry

    pairs = per_chunk // 2
    for i in range(CHUNKS):
        tile_copies[i].wait()
        if i + DEPTH < CHUNKS:
            tile_copies[i + DEPTH].start()
        lax.fori_loop(i * pairs, (i + 1) * pairs, pair, 0, unroll=UNROLL)

    picks[:, pl.ds(0, blocks)] = targets_ref[...]
    picks[:, pl.ds(blocks, blocks)] = targets_ref[...]
    picked = jnp.where(
        lax.broadcasted_iota(jnp.int32, (1, tile_count), 1) < blocks,
        picks[pl.ds(0, 1), :],
        picks[pl.ds(1, 1), :],
    )
    owner_ids = lax.broadcasted_iota(jnp.int32, (owners, tile_count), 0)
    selector = jnp.where(owner_ids == picked, 1.0, 0.0).astype(BF16)
    selector = jnp.concatenate([selector, selector], axis=1)

    air_rows[...] = jnp.zeros(air_rows.shape, F32)

    rows_in[:, pl.ds(dom, 1)] = rows_own[...].reshape(groups, 1, 1, 2 * air_cells)
    for k in peers:
        row_copy(k, peer(k)).wait_recv()

    rows = rows_in[...].reshape(owners, 2 * air_cells)
    fraction = rows[:, :air_cells]
    scale = fraction / rows[:, air_cells:]

    def gather(f, carry):
        right = []
        for q in range(lane_tiles):
            hi, lo = split(contrib[q, pl.ds(f, tile_count, stride=16), :])
            right.append(jnp.concatenate([hi, lo], axis=0))
        s = jnp.dot(selector, jnp.concatenate(right, axis=1), preferred_element_type=F32)
        summed[f] = s * scale
        air_rows[pl.ds(f, 1), :] = jnp.sum(s * fraction, axis=0, keepdims=True)
        return carry

    far = pl.ds(pl.multiple_of(other * domains, 8), domains)
    cuts = [(0, 8), (8, fields - 8)]
    pair_copies = []
    for n, (low, count) in enumerate(cuts):
        lax.fori_loop(low, low + count, gather, 0, unroll=4)
        part = pl.ds(low, count)
        copy = pltpu.make_async_remote_copy(
            src_ref=summed.at[part, far],
            dst_ref=partner_in.at[part],
            send_sem=pair_send.at[n],
            recv_sem=pair_recv.at[n],
            device_id=(other, dom),
            device_id_type=MESH,
        )
        copy.start()
        pair_copies.append(copy)
    ocean = fraction_ref[pl.ds(2, 1), :] * ocean_ref[...]
    air_num = jnp.sum(air_rows[pl.ds(0, fields), :] + air * ocean, axis=1, keepdims=True)
    air_den = jnp.sum(air)
    spot = lax.broadcasted_iota(jnp.int32, (fields, 128), 1)
    line = lax.broadcasted_iota(jnp.int32, (fields, 128), 0)
    stat = jnp.where(spot == line + 16 * comp, surface_num, 0.0)
    stat = stat + jnp.where(spot == line + 16 * groups, air_num, 0.0)
    stat = jnp.sum(stat, axis=0, keepdims=True)
    spot = lax.broadcasted_iota(jnp.int32, (1, 128), 1)
    dens = 16 * (groups + 1)
    stat = stat + jnp.where(spot == dens + comp, surface_den, 0.0)
    stat = stat + jnp.where(spot == dens + groups, air_den, 0.0)
    stat_out[...] = stat
    stat_pair = pltpu.make_async_remote_copy(
        src_ref=stat_out,
        dst_ref=stat_other,
        send_sem=stat_pair_send,
        recv_sem=stat_pair_recv,
        device_id=(other, dom),
        device_id_type=MESH,
    )
    stat_pair.start()

    def stat_copy(k, slot):
        return pltpu.make_async_remote_copy(
            src_ref=stat_sum,
            dst_ref=stat_in.at[slot],
            send_sem=stat_send.at[k],
            recv_sem=stat_recv.at[slot],
            device_id=(comp, peer(k)),
            device_id_type=MESH,
        )

    own = pl.ds(pl.multiple_of(comp * domains, 8), domains)

    def main_copy(n, k, slot):
        p = peer(k)
        return pltpu.make_async_remote_copy(
            src_ref=outgoing[n].at[p],
            dst_ref=incoming[n].at[slot],
            send_sem=main_send.at[n, k],
            recv_sem=main_recv.at[n, slot],
            device_id=(comp, p),
            device_id_type=MESH,
        )

    def send_group(n):
        low, count = cuts[n]
        pair_copies[n].wait()
        for f in range(low, low + count):
            outgoing[n][:, f - low, :] = summed[f, own, :] + partner_in[f]
        for k in peers:
            main_copy(n, k, dom).start()

    send_group(0)
    stat_pair.wait()
    stat = stat_out[...] + stat_other[...]
    stat_sum[...] = stat
    stat_in[dom] = stat
    for k in peers:
        stat_copy(k, dom).start()
    send_group(1)

    for n, (low, count) in enumerate(cuts):
        merged_ref[pl.ds(low, count), :] = ocean[low : low + count] + outgoing[n][dom]

    for n, (low, count) in enumerate(cuts):
        part = pl.ds(low, count)
        total = merged_ref[part, :]
        for k in peers:
            slot = peer(k)
            main_copy(n, k, slot).wait_recv()
            total = total + incoming[n][slot]
        merged_ref[part, :] = total
    for k in peers:
        stat_copy(k, peer(k)).wait_recv()

    stat = jnp.sum(stat_in[...], axis=0)
    for c in range(groups + 1):
        den = jnp.sum(jnp.where(spot == dens + c, stat, 0.0))
        moved = stat if c == 0 else pltpu.roll(stat, 128 - 16 * c, 1)
        means_ref[pl.ds(c, 1), :] = moved[:, :fields] / den

    for k in peers:
        row_copy(k, dom).wait_send()
        main_copy(0, k, dom).wait_send()
        main_copy(1, k, dom).wait_send()
        stat_copy(k, dom).wait_send()


def finish(merged_in, means_in, merged_ref, means_ref):
    merged_ref[...] = merged_in[...]
    means_ref[...] = means_in[...]


def on_device(
    surface_flux,
    active_mask,
    source_area,
    tile_targets,
    remap_tiles,
    ocean_flux,
    air_fraction,
    air_area,
):
    groups = lax.axis_size("comp")
    domains = lax.axis_size("dom")
    owners = groups * domains
    fields = surface_flux.shape[1]
    cells = surface_flux.shape[2]
    blocks, slots, block_cells, air_cells = remap_tiles.shape
    vmem = pl.BlockSpec(memory_space=pltpu.VMEM)
    hbm = pl.BlockSpec(memory_space=pl.ANY)
    dma = pltpu.SemaphoreType.DMA
    shapes = (
        jax.ShapeDtypeStruct((fields, air_cells), F32),
        jax.ShapeDtypeStruct((groups + 1, fields), F32),
    )
    parts = pl.pallas_call(
        functools.partial(kernel, groups, domains),
        out_shape=shapes,
        in_specs=[hbm, vmem, vmem, vmem, hbm, vmem, vmem, vmem],
        out_specs=(vmem, vmem),
        scratch_shapes=[
            pltpu.VMEM(surface_flux.shape, F32),
            pltpu.VMEM(remap_tiles.shape, F32),
            pltpu.VMEM((16, cells), F32),
            pltpu.VMEM((air_cells // 128, blocks * slots * 16, 128), F32),
            pltpu.VMEM((slots, blocks * slots), jnp.int32),
            pltpu.VMEM((groups, 1, 2 * air_cells), F32),
            pltpu.VMEM((groups, 1, 2 * air_cells), F32),
            pltpu.VMEM((groups, domains, 1, 2 * air_cells), F32),
            pltpu.VMEM((fields, owners, air_cells), F32),
            pltpu.VMEM((fields, domains, air_cells), F32),
            pltpu.VMEM((domains, 8, air_cells), F32),
            pltpu.VMEM((domains, fields - 8, air_cells), F32),
            pltpu.VMEM((domains, 8, air_cells), F32),
            pltpu.VMEM((domains, fields - 8, air_cells), F32),
            pltpu.VMEM((16, air_cells), F32),
            pltpu.VMEM((1, 128), F32),
            pltpu.VMEM((1, 128), F32),
            pltpu.VMEM((1, 128), F32),
            pltpu.VMEM((domains, 1, 128), F32),
            dma,
            dma((CHUNKS,)),
            dma,
            dma,
            dma((domains,)),
            dma((domains,)),
            dma,
            dma,
            dma((domains,)),
            dma((domains,)),
            dma((2,)),
            dma((2,)),
            dma((2, domains)),
            dma((2, domains)),
        ],
        compiler_params=pltpu.CompilerParams(
            collective_id=0, has_side_effects=True, vmem_limit_bytes=60 * 1024 * 1024
        ),
    )(
        surface_flux,
        active_mask.reshape(1, cells),
        source_area.reshape(1, cells),
        tile_targets.T,
        remap_tiles,
        ocean_flux,
        air_fraction,
        air_area,
    )
    return pl.pallas_call(
        finish, out_shape=shapes, in_specs=[vmem, vmem], out_specs=(vmem, vmem)
    )(*parts)


def solution(mesh):
    in_specs = (
        P(None, None, ("comp", "dom")),
        P(("comp", "dom")),
        P(("comp", "dom")),
        P(("comp", "dom"), None),
        P(("comp", "dom"), None, None, None),
        P(None, ("comp", "dom")),
        P(None, ("comp", "dom")),
        P(("comp", "dom")),
    )
    out_specs = (P(None, ("comp", "dom")), P())
    return jax.shard_map(
        on_device, mesh=mesh, in_specs=in_specs, out_specs=out_specs, check_vma=False
    )
```

```python
import functools

import jax
import jax.numpy as jnp
from jax import lax
from jax.experimental import pallas as pl
from jax.experimental.pallas import tpu as pltpu
from jax.sharding import PartitionSpec as P

MESH = pl.DeviceIdType.MESH
F32 = jnp.float32
BF16 = jnp.bfloat16
CHUNKS = 8
DEPTH = 4
UNROLL = 4


def split(x):
    hi = x.astype(BF16)
    lo = (x - hi.astype(F32)).astype(BF16)
    return hi, lo


def kernel(
    groups,
    domains,
    flux_hbm,
    mask_ref,
    area_ref,
    targets_ref,
    tiles_hbm,
    ocean_ref,
    fraction_ref,
    air_ref,
    merged_ref,
    means_ref,
    flux,
    tiles,
    weighted,
    contrib,
    picks,
    rows_out,
    rows_own,
    rows_in,
    summed,
    partner_in,
    outgoing_a,
    outgoing_b,
    incoming_a,
    incoming_b,
    air_rows,
    stat_out,
    stat_other,
    stat_sum,
    stat_in,
    flux_sem,
    tile_sem,
    row_pair_send,
    row_pair_recv,
    row_send,
    row_recv,
    stat_pair_send,
    stat_pair_recv,
    stat_send,
    stat_recv,
    pair_send,
    pair_recv,
    main_send,
    main_recv,
):
    steps, fields, cells = flux.shape
    blocks, slots, block_cells, air_cells = tiles.shape
    owners = groups * domains
    per_chunk = blocks // CHUNKS
    lane_tiles = air_cells // 128
    tile_count = blocks * slots
    comp = lax.axis_index("comp")
    dom = lax.axis_index("dom")
    other = 1 - comp
    outgoing = (outgoing_a, outgoing_b)
    incoming = (incoming_a, incoming_b)

    flux_copy = pltpu.make_async_copy(flux_hbm, flux, flux_sem)
    flux_copy.start()
    tile_copies = []
    for i in range(CHUNKS):
        part = pl.ds(i * per_chunk, per_chunk)
        copy = pltpu.make_async_copy(tiles_hbm.at[part], tiles.at[part], tile_sem.at[i])
        if i < DEPTH:
            copy.start()
        tile_copies.append(copy)

    barrier = pltpu.get_barrier_semaphore()

    def peer(k):
        p = dom + jnp.where(comp == 0, k, domains - k)
        return jnp.where(p >= domains, p - domains, p)

    peers = list(range(1, domains))
    pl.semaphore_signal(barrier, inc=1, device_id=(other, dom), device_id_type=MESH)
    for k in peers:
        pl.semaphore_signal(barrier, inc=1, device_id=(comp, peer(k)), device_id_type=MESH)

    air = air_ref[...].reshape(1, air_cells)
    for c in range(groups):
        rows_out[c, :, pl.ds(0, air_cells)] = fraction_ref[pl.ds(c, 1), :]
        rows_out[c, :, pl.ds(air_cells, air_cells)] = air
    rows_own[comp] = rows_out[comp]

    row_pair = pltpu.make_async_remote_copy(
        src_ref=rows_out.at[other],
        dst_ref=rows_own.at[comp],
        send_sem=row_pair_send,
        recv_sem=row_pair_recv,
        device_id=(other, dom),
        device_id_type=MESH,
    )

    def row_copy(k, slot):
        return pltpu.make_async_remote_copy(
            src_ref=rows_own,
            dst_ref=rows_in.at[:, slot],
            send_sem=row_send.at[k],
            recv_sem=row_recv.at[slot],
            device_id=(comp, peer(k)),
            device_id_type=MESH,
        )

    pl.semaphore_wait(barrier, domains)
    row_pair.start()
    row_pair.wait()
    for k in peers:
        row_copy(k, dom).start()
    flux_copy.wait()
    weighted[pl.ds(8, 8), :] = jnp.zeros((8, cells), F32)
    width = 512

    def weigh(i, carry):
        total, area_total = carry
        part = pl.ds(pl.multiple_of(i * width, width), width)
        value = flux[0, :, part]
        for s in range(1, steps):
            value = value + flux[s, :, part]
        area = area_ref[:, part]
        value = (value / steps) * (mask_ref[:, part].astype(F32) * area)
        weighted[pl.ds(0, fields), part] = value
        return total + value, area_total + area

    total, area_total = lax.fori_loop(
        0,
        cells // width,
        weigh,
        (jnp.zeros((fields, width), F32), jnp.zeros((1, width), F32)),
        unroll=2,
    )
    surface_num = jnp.sum(total, axis=1, keepdims=True)
    surface_den = jnp.sum(area_total)

    lane = lax.broadcasted_iota(jnp.int32, (16, 128), 1)
    first = lane < block_cells
    blank = jnp.zeros((16, 128), BF16)

    def pair(j, carry):
        cell = pl.ds(pl.multiple_of(j * 128, 128), 128)
        w = weighted[:, cell]
        lhs = []
        for keep in (first, ~first):
            hi, lo = split(jnp.where(keep, w, 0.0))
            lhs.append(jnp.concatenate([hi, hi], axis=1))
            lhs.append(jnp.concatenate([lo, blank], axis=1))
        left = jnp.concatenate(lhs, axis=0)
        for t in range(slots):
            weights = tiles[pl.ds(2 * j, 2), t].reshape(2 * block_cells, air_cells)
            hi, lo = split(weights)
            right = jnp.concatenate([hi, lo], axis=0)
            r = jnp.dot(left, right, preferred_element_type=F32)
            even = r[0:16] + r[16:32]
            odd = r[32:48] + r[48:64]
            base = pl.multiple_of((t * blocks + 2 * j) * 16, 32)
            for q in range(lane_tiles):
                cut = slice(q * 128, (q + 1) * 128)
                contrib[q, pl.ds(base, 16), :] = even[:, cut]
                contrib[q, pl.ds(base + 16, 16), :] = odd[:, cut]
        return carry

    pairs = per_chunk // 2
    for i in range(CHUNKS):
        tile_copies[i].wait()
        if i + DEPTH < CHUNKS:
            tile_copies[i + DEPTH].start()
        lax.fori_loop(i * pairs, (i + 1) * pairs, pair, 0, unroll=UNROLL)

    picks[:, pl.ds(0, blocks)] = targets_ref[...]
    picks[:, pl.ds(blocks, blocks)] = targets_ref[...]
    picked = jnp.where(
        lax.broadcasted_iota(jnp.int32, (1, tile_count), 1) < blocks,
        picks[pl.ds(0, 1), :],
        picks[pl.ds(1, 1), :],
    )
    owner_ids = lax.broadcasted_iota(jnp.int32, (owners, tile_count), 0)
    selector = jnp.where(owner_ids == picked, 1.0, 0.0).astype(BF16)
    selector = jnp.concatenate([selector, selector], axis=1)

    air_rows[...] = jnp.zeros(air_rows.shape, F32)

    def collect(f, carry):
        right = []
        for q in range(lane_tiles):
            hi, lo = split(contrib[q, pl.ds(f, tile_count, stride=16), :])
            right.append(jnp.concatenate([hi, lo], axis=0))
        s = jnp.dot(selector, jnp.concatenate(right, axis=1), preferred_element_type=F32)
        summed[f] = s
        return carry

    lax.fori_loop(0, 8, collect, 0, unroll=4)

    rows_in[:, pl.ds(dom, 1)] = rows_own[...].reshape(groups, 1, 1, 2 * air_cells)
    for k in peers:
        row_copy(k, peer(k)).wait_recv()

    rows = rows_in[...].reshape(owners, 2 * air_cells)
    fraction = rows[:, :air_cells]
    scale = fraction / rows[:, air_cells:]

    def weigh_sums(f, carry):
        s = summed[f]
        summed[f] = s * scale
        air_rows[pl.ds(f, 1), :] = jnp.sum(s * fraction, axis=0, keepdims=True)
        return carry

    far = pl.ds(pl.multiple_of(other * domains, 8), domains)
    cuts = [(0, 8), (8, fields - 8)]
    pair_copies = []
    for n, (low, count) in enumerate(cuts):
        if n > 0:
            lax.fori_loop(low, low + count, collect, 0, unroll=4)
        lax.fori_loop(low, low + count, weigh_sums, 0, unroll=4)
        part = pl.ds(low, count)
        copy = pltpu.make_async_remote_copy(
            src_ref=summed.at[part, far],
            dst_ref=partner_in.at[part],
            send_sem=pair_send.at[n],
            recv_sem=pair_recv.at[n],
            device_id=(other, dom),
            device_id_type=MESH,
        )
        copy.start()
        pair_copies.append(copy)
    ocean = fraction_ref[pl.ds(2, 1), :] * ocean_ref[...]
    air_num = jnp.sum(air_rows[pl.ds(0, fields), :] + air * ocean, axis=1, keepdims=True)
    air_den = jnp.sum(air)
    spot = lax.broadcasted_iota(jnp.int32, (fields, 128), 1)
    line = lax.broadcasted_iota(jnp.int32, (fields, 128), 0)
    stat = jnp.where(spot == line + 16 * comp, surface_num, 0.0)
    stat = stat + jnp.where(spot == line + 16 * groups, air_num, 0.0)
    stat = jnp.sum(stat, axis=0, keepdims=True)
    spot = lax.broadcasted_iota(jnp.int32, (1, 128), 1)
    dens = 16 * (groups + 1)
    stat = stat + jnp.where(spot == dens + comp, surface_den, 0.0)
    stat = stat + jnp.where(spot == dens + groups, air_den, 0.0)
    stat_out[...] = stat
    stat_pair = pltpu.make_async_remote_copy(
        src_ref=stat_out,
        dst_ref=stat_other,
        send_sem=stat_pair_send,
        recv_sem=stat_pair_recv,
        device_id=(other, dom),
        device_id_type=MESH,
    )
    stat_pair.start()

    def stat_copy(k, slot):
        return pltpu.make_async_remote_copy(
            src_ref=stat_sum,
            dst_ref=stat_in.at[slot],
            send_sem=stat_send.at[k],
            recv_sem=stat_recv.at[slot],
            device_id=(comp, peer(k)),
            device_id_type=MESH,
        )

    own = pl.ds(pl.multiple_of(comp * domains, 8), domains)

    def main_copy(n, k, slot):
        p = peer(k)
        return pltpu.make_async_remote_copy(
            src_ref=outgoing[n].at[p],
            dst_ref=incoming[n].at[slot],
            send_sem=main_send.at[n, k],
            recv_sem=main_recv.at[n, slot],
            device_id=(comp, p),
            device_id_type=MESH,
        )

    def send_group(n):
        low, count = cuts[n]
        pair_copies[n].wait()
        for f in range(low, low + count):
            outgoing[n][:, f - low, :] = summed[f, own, :] + partner_in[f]
        for k in peers:
            main_copy(n, k, dom).start()

    send_group(0)
    stat_pair.wait()
    stat = stat_out[...] + stat_other[...]
    stat_sum[...] = stat
    stat_in[dom] = stat
    for k in peers:
        stat_copy(k, dom).start()
    send_group(1)

    for n, (low, count) in enumerate(cuts):
        merged_ref[pl.ds(low, count), :] = ocean[low : low + count] + outgoing[n][dom]

    for n, (low, count) in enumerate(cuts):
        part = pl.ds(low, count)
        total = merged_ref[part, :]
        for k in peers:
            slot = peer(k)
            main_copy(n, k, slot).wait_recv()
            total = total + incoming[n][slot]
        merged_ref[part, :] = total
    for k in peers:
        stat_copy(k, peer(k)).wait_recv()

    stat = jnp.sum(stat_in[...], axis=0)
    for c in range(groups + 1):
        den = jnp.sum(jnp.where(spot == dens + c, stat, 0.0))
        moved = stat if c == 0 else pltpu.roll(stat, 128 - 16 * c, 1)
        means_ref[pl.ds(c, 1), :] = moved[:, :fields] / den

    for k in peers:
        row_copy(k, dom).wait_send()
        main_copy(0, k, dom).wait_send()
        main_copy(1, k, dom).wait_send()
        stat_copy(k, dom).wait_send()


def finish(merged_in, means_in, merged_ref, means_ref):
    merged_ref[...] = merged_in[...]
    means_ref[...] = means_in[...]


def on_device(
    surface_flux,
    active_mask,
    source_area,
    tile_targets,
    remap_tiles,
    ocean_flux,
    air_fraction,
    air_area,
):
    groups = lax.axis_size("comp")
    domains = lax.axis_size("dom")
    owners = groups * domains
    fields = surface_flux.shape[1]
    cells = surface_flux.shape[2]
    blocks, slots, block_cells, air_cells = remap_tiles.shape
    vmem = pl.BlockSpec(memory_space=pltpu.VMEM)
    hbm = pl.BlockSpec(memory_space=pl.ANY)
    dma = pltpu.SemaphoreType.DMA
    shapes = (
        jax.ShapeDtypeStruct((fields, air_cells), F32),
        jax.ShapeDtypeStruct((groups + 1, fields), F32),
    )
    parts = pl.pallas_call(
        functools.partial(kernel, groups, domains),
        out_shape=shapes,
        in_specs=[hbm, vmem, vmem, vmem, hbm, vmem, vmem, vmem],
        out_specs=(vmem, vmem),
        scratch_shapes=[
            pltpu.VMEM(surface_flux.shape, F32),
            pltpu.VMEM(remap_tiles.shape, F32),
            pltpu.VMEM((16, cells), F32),
            pltpu.VMEM((air_cells // 128, blocks * slots * 16, 128), F32),
            pltpu.VMEM((slots, blocks * slots), jnp.int32),
            pltpu.VMEM((groups, 1, 2 * air_cells), F32),
            pltpu.VMEM((groups, 1, 2 * air_cells), F32),
            pltpu.VMEM((groups, domains, 1, 2 * air_cells), F32),
            pltpu.VMEM((fields, owners, air_cells), F32),
            pltpu.VMEM((fields, domains, air_cells), F32),
            pltpu.VMEM((domains, 8, air_cells), F32),
            pltpu.VMEM((domains, fields - 8, air_cells), F32),
            pltpu.VMEM((domains, 8, air_cells), F32),
            pltpu.VMEM((domains, fields - 8, air_cells), F32),
            pltpu.VMEM((16, air_cells), F32),
            pltpu.VMEM((1, 128), F32),
            pltpu.VMEM((1, 128), F32),
            pltpu.VMEM((1, 128), F32),
            pltpu.VMEM((domains, 1, 128), F32),
            dma,
            dma((CHUNKS,)),
            dma,
            dma,
            dma((domains,)),
            dma((domains,)),
            dma,
            dma,
            dma((domains,)),
            dma((domains,)),
            dma((2,)),
            dma((2,)),
            dma((2, domains)),
            dma((2, domains)),
        ],
        compiler_params=pltpu.CompilerParams(
            collective_id=0, has_side_effects=True, vmem_limit_bytes=60 * 1024 * 1024
        ),
    )(
        surface_flux,
        active_mask.reshape(1, cells),
        source_area.reshape(1, cells),
        tile_targets.T,
        remap_tiles,
        ocean_flux,
        air_fraction,
        air_area,
    )
    return pl.pallas_call(
        finish, out_shape=shapes, in_specs=[vmem, vmem], out_specs=(vmem, vmem)
    )(*parts)


def solution(mesh):
    in_specs = (
        P(None, None, ("comp", "dom")),
        P(("comp", "dom")),
        P(("comp", "dom")),
        P(("comp", "dom"), None),
        P(("comp", "dom"), None, None, None),
        P(None, ("comp", "dom")),
        P(None, ("comp", "dom")),
        P(("comp", "dom")),
    )
    out_specs = (P(None, ("comp", "dom")), P())
    return jax.shard_map(
        on_device, mesh=mesh, in_specs=in_specs, out_specs=out_specs, check_vma=False
    )
```
